32 devices in a mesh: dp: 1 (over z), fsdp: 4 (over y), ep: 8 (over x, core).
Axes of the slice: x: 4, y: 4, z: 1, core: 2. Of those that a mesh axis runs over, the one named last changes fastest.
The devices are a block of a 4x4x8 slice.
Arguments:
- hidden: bfloat16 [131072, 1024], P(('dp', 'fsdp', 'ep'))
- norm_gain: bfloat16 [1024], replicated
- w_router: bfloat16 [1024, 32], replicated
- w_gate: bfloat16 [32, 1024, 2816], P('ep', 'fsdp')
- w_up: bfloat16 [32, 1024, 2816], P('ep', 'fsdp')
- w_down: bfloat16 [32, 2816, 1024], P('ep', None, 'fsdp')
- top2_ids: int32 [131072, 2], P(('dp', 'fsdp', 'ep'))
Outputs:
- output: bfloat16 [131072, 1024], P(('dp', 'fsdp', 'ep'))
All inputs are finite; a program needn't handle non-finite values.
Results may differ from the reference program's by a relative error of at most 0.001.
Values are sent between devices in bfloat16 or wider.
A program may use at most 768 MiB of HBM per device.

```python
import jax
import jax.numpy as jnp
import numpy as np
from jax import lax

D = 1024
FF = 2816
EXPERTS = 32
TOKENS_DEV = 4096
GROUPS = 32
TOKENS = GROUPS * TOKENS_DEV
CAPACITY = (5 * TOKENS_DEV + 2 * EXPERTS - 1) // (2 * EXPERTS)
EPS = 1e-5


def draw_routes(route_key):
    perm_key, first_key, second_key = jax.random.split(route_key, 3)
    hot_count = max(EXPERTS // 4, 1)
    route_table = jnp.asarray(np.repeat(np.arange(EXPERTS), np.where(np.arange(EXPERTS) < hot_count, 4, 1)), dtype=jnp.int32)
    expert_perm = jax.random.permutation(perm_key, EXPERTS)
    table_pick = jax.random.randint(first_key, (TOKENS,), 0, route_table.shape[0])
    local_index = jnp.arange(TOKENS, dtype=jnp.int32) % TOKENS_DEV
    first_choice = jnp.where(local_index < EXPERTS, local_index, expert_perm[route_table[table_pick]])
    second_shift = jax.random.randint(second_key, (TOKENS,), 1, EXPERTS)
    second_choice = (first_choice + second_shift) % EXPERTS
    return jnp.stack([first_choice, second_choice], axis=1).astype(jnp.int32)


def setup_inputs(seed: int = 0, part: int = 0) -> dict:
    part_key = jax.random.fold_in(jax.random.key(seed), part)
    hidden_key, route_key = jax.random.split(part_key, 2)
    gain_key, router_key, gate_key, up_key, down_key = jax.random.split(jax.random.key(seed + 1), 5)
    hidden = jax.random.normal(hidden_key, (TOKENS, D), jnp.float32)
    norm_gain = jax.random.uniform(gain_key, (D,), jnp.float32, 0.5, 1.5)
    w_router = jax.random.normal(router_key, (D, EXPERTS), jnp.float32) * (0.5 * D ** -0.5)
    w_gate = jax.random.normal(gate_key, (EXPERTS, D, FF), jnp.float32) * D ** -0.5
    w_up = jax.random.normal(up_key, (EXPERTS, D, FF), jnp.float32) * D ** -0.5
    w_down = jax.random.normal(down_key, (EXPERTS, FF, D), jnp.float32) * FF ** -0.5
    return {
        'hidden': hidden.astype(jnp.bfloat16),
        'norm_gain': norm_gain.astype(jnp.bfloat16),
        'w_router': w_router.astype(jnp.bfloat16),
        'w_gate': w_gate.astype(jnp.bfloat16),
        'w_up': w_up.astype(jnp.bfloat16),
        'w_down': w_down.astype(jnp.bfloat16),
        'top2_ids': draw_routes(route_key),
    }


def expert_ffn(expert_pack):
    rows_in, gate_mat, up_mat, down_mat = expert_pack
    act_a = jnp.dot(rows_in, gate_mat, preferred_element_type=jnp.float32)
    act_b = jnp.dot(rows_in, up_mat, preferred_element_type=jnp.float32)
    hidden_act = (jax.nn.silu(act_a) * act_b).astype(jnp.bfloat16)
    return jnp.dot(hidden_act, down_mat, preferred_element_type=jnp.float32).astype(jnp.bfloat16)


def reference(hidden, norm_gain, w_router, w_gate, w_up, w_down, top2_ids):
    hidden_f32 = hidden.astype(jnp.float32)
    mean_sq = jnp.mean(hidden_f32 * hidden_f32, axis=-1, keepdims=True)
    normed = (hidden_f32 * lax.rsqrt(mean_sq + EPS) * norm_gain.astype(jnp.float32)).astype(jnp.bfloat16)
    logits = jnp.dot(normed, w_router, preferred_element_type=jnp.float32)
    gate_probs = jax.nn.softmax(jnp.take_along_axis(logits, top2_ids, axis=1), axis=-1)
    flat_ids = top2_ids.reshape(GROUPS, 2 * TOKENS_DEV)
    onehot = (flat_ids[:, :, None] == jnp.arange(EXPERTS, dtype=jnp.int32)).astype(jnp.int32)
    position = jnp.sum((jnp.cumsum(onehot, axis=1) - 1) * onehot, axis=2)
    group_base = jnp.arange(GROUPS, dtype=jnp.int32)[:, None] * (EXPERTS * CAPACITY)
    all_slots = GROUPS * EXPERTS * CAPACITY
    slot_ids = jnp.where(position < CAPACITY, group_base + flat_ids * CAPACITY + position, all_slots).reshape(TOKENS, 2)
    token_index = jnp.broadcast_to(jnp.arange(TOKENS, dtype=jnp.int32)[:, None], (TOKENS, 2))
    source = jnp.full((all_slots,), TOKENS, dtype=jnp.int32).at[slot_ids.reshape(-1)].set(token_index.reshape(-1), mode='drop')
    buffers = jnp.take(normed, source, axis=0, mode='fill', fill_value=0)
    by_expert = buffers.reshape(GROUPS, EXPERTS, CAPACITY, D).transpose(1, 0, 2, 3).reshape(EXPERTS, GROUPS * CAPACITY, D)
    expert_out = lax.map(expert_ffn, (by_expert, w_gate, w_up, w_down))
    out_flat = expert_out.reshape(EXPERTS, GROUPS, CAPACITY, D).transpose(1, 0, 2, 3).reshape(all_slots, D)
    returned = jnp.take(out_flat, slot_ids, axis=0, mode='fill', fill_value=0)
    moe_sum = jnp.sum(gate_probs[:, :, None] * returned.astype(jnp.float32), axis=1)
    return (hidden_f32 + moe_sum).astype(jnp.bfloat16)
```

```python
import functools
from typing import NamedTuple

import jax
import jax.numpy as jnp
from jax import lax
from jax.experimental import pallas as pl
from jax.experimental.pallas import tpu as pltpu
from jax.sharding import PartitionSpec as P

EPS = 1e-5
TILE = 256
WIN = 64
ALIGN = 16
VMEM_LIMIT = 60 * 1024 * 1024


def norm_and_gates(hidden, norm_gain, w_router, top2_ids):
    hidden_f32 = hidden.astype(jnp.float32)
    mean_sq = jnp.mean(hidden_f32 * hidden_f32, axis=-1, keepdims=True)
    normed = (hidden_f32 * lax.rsqrt(mean_sq + EPS) * norm_gain.astype(jnp.float32)).astype(jnp.bfloat16)
    logits = jnp.dot(normed, w_router, preferred_element_type=jnp.float32)
    experts = jnp.arange(w_router.shape[1], dtype=jnp.int32)[None, :]
    picked = [jnp.sum(jnp.where(top2_ids[:, k:k + 1] == experts, logits, 0.0), axis=1) for k in range(2)]
    gate_probs = jax.nn.softmax(jnp.stack(picked, axis=1), axis=-1)
    return normed, gate_probs


def route(top2_ids, num_experts, capacity):
    tok_count = top2_ids.shape[0]
    experts = jnp.arange(num_experts, dtype=jnp.int32)[None, :]
    hit0 = top2_ids[:, 0:1] == experts
    hit1 = top2_ids[:, 1:2] == experts
    chosen = (hit0 | hit1).astype(jnp.bfloat16)
    block = 128
    blocks = chosen.reshape(tok_count // block, block, num_experts)
    strict = (jnp.arange(block)[:, None] > jnp.arange(block)[None, :]).astype(jnp.bfloat16)
    inside = jnp.einsum('st,bte->bse', strict, blocks, preferred_element_type=jnp.float32)
    totals = jnp.sum(blocks.astype(jnp.float32), axis=1)
    count = tok_count // block
    before = jnp.sum(jnp.where((jnp.arange(count)[:, None] > jnp.arange(count)[None, :])[:, :, None], totals[None], 0.0), axis=1)
    rank = (inside + before[:, None, :]).reshape(tok_count, num_experts).astype(jnp.int32)
    slots = []
    for k, hit in enumerate((hit0, hit1)):
        pos = jnp.sum(jnp.where(hit, rank, 0), axis=1)
        slots.append(jnp.where(pos < capacity, top2_ids[:, k] * capacity + pos, -1))
    kept = (hit0 | hit1) & (rank < capacity)
    per_expert = jnp.where(kept, rank, -1).T
    step = TILE // block
    starts = jnp.concatenate([before[::step], (before[-1:] + totals[-1:])], axis=0)
    starts = jnp.minimum(starts.astype(jnp.int32), capacity)
    return slots, per_expert, starts


def window(starts_ref, tile, expert, round_idx, capacity):
    first = starts_ref[tile, expert] // ALIGN * ALIGN + round_idx * WIN
    base = jnp.minimum(first, capacity - WIN)
    return pl.multiple_of(base, ALIGN), first


def round_count(starts_ref, tile, experts, capacity):
    need = jnp.int32(0)
    for expert in experts:
        low = starts_ref[tile, expert] // ALIGN * ALIGN
        need = jnp.maximum(need, starts_ref[tile + 1, expert] - low)
    return (need + WIN - 1) // WIN


def combine_kernel(experts, local, capacity, count, starts_ref, tok_ref, acc_ref, *refs):
    rets, out_ref, stage, total = refs[:count], refs[count], refs[count + 1], refs[count + 2]
    tile = pl.program_id(0)
    total[...] = acc_ref[...].astype(jnp.float32)
    width = 8 * WIN
    lane = lax.broadcasted_iota(jnp.int32, (1, width), 1)
    which = lane // WIN
    inner = lane % WIN

    def one_round(round_idx, carry):
        for g in range(0, len(experts), 8):
            slot = jnp.zeros((1, width), jnp.int32)
            valid = jnp.zeros((1, width), jnp.int32)
            for i, e in enumerate(experts[g:g + 8]):
                base, first = window(starts_ref, tile, e, round_idx, capacity)
                stage[i * WIN:(i + 1) * WIN, :] = rets[0][e % local, e // local, pl.ds(base, WIN), :]
                slot = jnp.where(which == i, e * capacity + base, slot)
                valid = jnp.where(which == i, e * capacity + first, valid)
            slot = slot + inner
            slot = jnp.where(slot >= valid, slot, -2).astype(jnp.float32)
            for k in range(2):
                pick = jnp.where(tok_ref[:, k:k + 1] == slot, 1.0, 0.0).astype(jnp.bfloat16)
                got = jnp.dot(pick, stage[...], preferred_element_type=jnp.float32)
                total[...] += tok_ref[:, 2 + k:3 + k] * got
        return carry

    lax.fori_loop(0, round_count(starts_ref, tile, experts, capacity), one_round, 0)
    out_ref[...] = total[...].astype(out_ref.dtype)


def combine(acc, rets, indices, tok, starts, num_experts, capacity, local, out_dtype):
    tok_count, d_model = acc.shape
    dests = num_experts // local
    experts = [j * local + i for i in indices for j in range(dests)]
    shape = rets[0].shape
    return pl.pallas_call(
        functools.partial(combine_kernel, experts, local, capacity, len(rets)),
        out_shape=jax.ShapeDtypeStruct(acc.shape, out_dtype),
        grid_spec=pltpu.PrefetchScalarGridSpec(
            num_scalar_prefetch=1,
            grid=(tok_count // TILE,),
            in_specs=[
                pl.BlockSpec((TILE, 4), lambda t, s: (t, 0)),
                pl.BlockSpec((TILE, d_model), lambda t, s: (t, 0)),
            ] + [pl.BlockSpec(shape, lambda t, s: (0, 0, 0, 0), pipeline_mode=pl.Buffered(1))] * len(rets),
            out_specs=pl.BlockSpec((TILE, d_model), lambda t, s: (t, 0)),
            scratch_shapes=[pltpu.VMEM((8 * WIN, d_model), jnp.bfloat16), pltpu.VMEM((TILE, d_model), jnp.float32)],
        ),
        compiler_params=pltpu.CompilerParams(dimension_semantics=('arbitrary',), vmem_limit_bytes=VMEM_LIMIT),
        cost_estimate=pl.CostEstimate(flops=4 * tok_count * len(experts) * WIN * d_model, bytes_accessed=8 * tok_count * d_model, transcendentals=0),
        name='combine_rows',
    )(starts, tok, acc, *rets)


class Unit(NamedTuple):
    expert: int
    kind: int
    low: int
    size: int


GATE, UP, DOWN = 0, 1, 2
MESH = pl.DeviceIdType.MESH
AHEAD = 3
FFB = 256


def unit_list(local, ff):
    units = []
    cuts = [0, 1024, 2048, ff]
    for e in range(local):
        if e < local - 1:
            units += [Unit(e, GATE, 0, ff), Unit(e, UP, 0, ff)]
        else:
            for low, high in zip(cuts[:-1], cuts[1:]):
                units += [Unit(e, GATE, low, high - low), Unit(e, UP, low, high - low)]
        units.append(Unit(e, DOWN, 0, ff))
    return units


def moe_kernel(units, capacity, slots_ref, normed_hbm, gate_hbm, up_hbm, down_hbm,
               ret_hbm, send_hbm, recv_hbm, out_hbm, gate_all, up_all, down_all,
               normed, stage, rows, act, wbuf, dbuf, obuf,
               w_send, w_recv, a_send, a_recv, r_send, r_recv, c_send, c_recv,
               normed_sem, stage_sem, rows_sem, wbuf_sem, dbuf_sem, obuf_sem):
    local, d_shard, ff = gate_hbm.shape
    fsdp = gate_all.shape[1]
    dests = recv_hbm.shape[1]
    f_me, j_me = lax.axis_index('fsdp'), lax.axis_index('ep')
    right, left, far = lax.rem(f_me + 1, fsdp), lax.rem(f_me + fsdp - 1, fsdp), lax.rem(f_me + 2, fsdp)
    last = local - 1
    index = {(u.expert, u.kind, u.low): c for c, u in enumerate(units)}

    barrier = pltpu.get_barrier_semaphore()
    pl.semaphore_signal(barrier, inc=1, device_id={'fsdp': right}, device_id_type=MESH)
    pl.semaphore_signal(barrier, inc=1, device_id={'fsdp': left}, device_id_type=MESH)
    for step in range(1, dests):
        pl.semaphore_signal(barrier, inc=1, device_id={'ep': lax.rem(j_me + step, dests)}, device_id_type=MESH)
    pl.semaphore_wait(barrier, 2 + dests - 1)

    def own_part(u):
        if u.kind == DOWN:
            return down_hbm.at[u.expert]
        return (gate_hbm, up_hbm)[u.kind].at[u.expert, :, pl.ds(u.low, u.size)]

    def all_part(u, f, half=None):
        if u.kind == DOWN:
            span = pl.ds(0, ff) if half is None else pl.ds(half * (ff // 2), ff // 2)
            return down_all.at[u.expert, f, span, :]
        span = pl.ds(0, d_shard) if half is None else pl.ds(half * (d_shard // 2), d_shard // 2)
        return (gate_all, up_all)[u.kind].at[u.expert, f, span, pl.ds(u.low, u.size)]

    def direct(c, way):
        u = units[c]
        return pltpu.make_async_remote_copy(
            src_ref=own_part(u), dst_ref=all_part(u, f_me), send_sem=w_send.at[c, way], recv_sem=w_recv.at[c, way],
            device_id={'fsdp': (right, left)[way]}, device_id_type=MESH)

    def forward(c, way):
        u = units[c]
        part = all_part(u, (left, right)[way], way)
        return pltpu.make_async_remote_copy(
            src_ref=part, dst_ref=part, send_sem=w_send.at[c, 2 + way], recv_sem=w_recv.at[c, 2 + way],
            device_id={'fsdp': (right, left)[way]}, device_id_type=MESH)

    def start_direct(c):
        for way in range(2):
            direct(c, way).start()

    def service(c, then):
        for way in range(2):
            direct(c, way).wait_recv()
            forward(c, way).start()
        for n in then:
            start_direct(n)

    def wait_far(c):
        for way in range(2):
            forward(c, way).wait_recv()

    for c in range(AHEAD):
        start_direct(c)
    load = pltpu.make_async_copy(normed_hbm, normed, normed_sem)
    load.start()
    load.wait()

    def dest_of(step):
        return lax.rem(j_me + 1 + step, dests)

    def store_rows(i, step):
        slot = lax.rem(step, 2)
        return pltpu.make_async_copy(stage.at[slot], send_hbm.at[i, dest_of(step)], stage_sem.at[slot])

    def send_rows(i, step):
        j = dest_of(step)
        return pltpu.make_async_remote_copy(
            src_ref=send_hbm.at[i, j], dst_ref=recv_hbm.at[i, j_me], send_sem=a_send.at[i, step], recv_sem=a_recv.at[i, j_me],
            device_id={'ep': j}, device_id_type=MESH)

    row_iota = lax.broadcasted_iota(jnp.int32, (capacity, normed.shape[0]), 0)

    def dispatch(i):
        def body(step, carry):
            want = slots_ref[pl.ds(dest_of(step) * local + i, 1), :]
            pick = jnp.where(row_iota == want, 1.0, 0.0).astype(jnp.bfloat16)
            stage[lax.rem(step, 2)] = jnp.dot(pick, normed[...], preferred_element_type=jnp.float32).astype(jnp.bfloat16)

            @pl.when(step > 0)
            def _():
                store_rows(i, step - 1).wait()
                send_rows(i, step - 1).start()

            store_rows(i, step).start()
            return carry

        lax.fori_loop(0, dests, body, 0)
        store_rows(i, dests - 1).wait()

    def load_rows(e):
        def copy(step):
            j = dest_of(step)
            if step == dests - 1:
                return pltpu.make_async_copy(send_hbm.at[e, j], rows.at[j], rows_sem.at[step])
            return pltpu.make_async_copy(recv_hbm.at[e, j], rows.at[j], rows_sem.at[step])

        for step in range(dests - 1):
            j = dest_of(step)
            pltpu.make_async_remote_copy(
                src_ref=send_hbm.at[e, j], dst_ref=recv_hbm.at[e, j], send_sem=a_send.at[e, step], recv_sem=a_recv.at[e, j],
                device_id={'ep': j}, device_id_type=MESH).wait_recv()
        for step in range(dests):
            copy(step).start()
        for step in range(dests):
            copy(step).wait()

    def block_copies(e, b, slot):
        cols = pl.ds(pl.multiple_of(b * FFB, FFB), FFB)
        copies = []
        for m, (own, whole) in enumerate(((gate_hbm, gate_all), (up_hbm, up_all))):
            for r in range(fsdp):
                f = lax.rem(f_me + r, fsdp)
                src = own.at[e, :, cols] if r == 0 else whole.at[e, f, :, cols]
                copies.append(pltpu.make_async_copy(src, wbuf.at[slot, m, f], wbuf_sem.at[slot, m, r]))
        return copies

    def phase_one(e, low, high):
        for copy in block_copies(e, low, low % 2):
            copy.start()

        def body(b, carry):
            slot = lax.rem(b, 2)

            @pl.when(b + 1 < high)
            def _():
                for copy in block_copies(e, b + 1, 1 - slot):
                    copy.start()

            for copy in block_copies(e, b, slot):
                copy.wait()
            gate = wbuf[slot, GATE].reshape(fsdp * d_shard, FFB)
            up = wbuf[slot, UP].reshape(fsdp * d_shard, FFB)
            for r in range(dests // 2):
                x = rows[2 * r:2 * r + 2].reshape(2 * capacity, fsdp * d_shard)
                a = jnp.dot(x, gate, preferred_element_type=jnp.float32)
                u = jnp.dot(x, up, preferred_element_type=jnp.float32)
                act[2 * r * capacity:(2 * r + 2) * capacity, pl.ds(pl.multiple_of(b * FFB, FFB), FFB)] = (a * jax.nn.sigmoid(a) * u).astype(jnp.bfloat16)
            return carry

        lax.fori_loop(low, high, body, 0)

    def back_rows(e, step):
        j = dest_of(step)
        return pltpu.make_async_remote_copy(
            src_ref=out_hbm.at[e, j], dst_ref=ret_hbm.at[e, j_me], send_sem=r_send.at[e, step], recv_sem=r_recv.at[e, j_me],
            device_id={'ep': j}, device_id_type=MESH)

    def back_cols(n, f, step):
        j = dest_of(step)
        cols = pl.ds(pl.multiple_of(f * d_shard, d_shard), d_shard)
        return pltpu.make_async_remote_copy(
            src_ref=out_hbm.at[last, j, :, cols], dst_ref=ret_hbm.at[last, j_me, :, cols], send_sem=c_send.at[n, step], recv_sem=c_recv.at[f, j_me],
            device_id={'ep': j}, device_id_type=MESH)

    order = (f_me, left, right, far)

    def down_load(e, n):
        src = down_hbm.at[e] if n == 0 else down_all.at[e, order[n]]
        return pltpu.make_async_copy(src, dbuf.at[n % 2], dbuf_sem.at[n % 2])

    def down_column(e, n):
        f = order[n]

        def body(r, carry):
            hid = act[pl.ds(pl.multiple_of(r * 2 * capacity, 2 * capacity), 2 * capacity), :]
            got = jnp.dot(hid, dbuf[n % 2], preferred_element_type=jnp.float32).astype(jnp.bfloat16)
            obuf[pl.ds(2 * r, 2)] = got.reshape(2, capacity, d_shard)
            return carry

        lax.fori_loop(0, dests // 2, body, 0)
        cols = pl.ds(pl.multiple_of(f * d_shard, d_shard), d_shard)
        mine = pltpu.make_async_copy(obuf.at[j_me], ret_hbm.at[e, j_me, :, cols], obuf_sem.at[0])
        rest = pltpu.make_async_copy(obuf, out_hbm.at[e, :, :, cols], obuf_sem.at[1])
        mine.start()
        rest.start()
        mine.wait()
        rest.wait()

    def phase_two(e, far_unit):
        down_load(e, 0).start()
        down_load(e, 1).start()
        down_load(e, 0).wait()
        down_column(e, 0)
        if e == last:
            for step in range(dests - 1):
                back_cols(0, order[0], step).start()
        down_load(e, 2).start()
        down_load(e, 1).wait()
        down_column(e, 1)
        if e == last:
            for step in range(dests - 1):
                back_cols(1, order[1], step).start()
        down_load(e, 2).wait()
        down_column(e, 2)
        if e == last:
            for step in range(dests - 1):
                back_cols(2, order[2], step).start()
        wait_far(far_unit)
        down_load(e, 3).start()
        down_load(e, 3).wait()
        down_column(e, 3)
        for step in range(dests - 1):
            if e == last:
                back_cols(3, order[3], step).start()
            else:
                back_rows(e, step).start()

    first_last = index[last, GATE, 0]
    final = index[last, DOWN, 0]

    def then(c):
        n = c + AHEAD
        if n < final:
            return (n,)
        return (final,) if c == final - 1 else ()

    done = 0

    def serve(upto):
        nonlocal done
        while done <= upto:
            service(done, then(done))
            done += 1

    for i in range(local):
        dispatch(i)
        if i < local - 1:
            serve(i)
    blocks = ff // FFB
    for e in range(last):
        g = index[e, GATE, 0]
        serve(g + 3)
        wait_far(g)
        wait_far(g + 1)
        load_rows(e)
        phase_one(e, 0, blocks)
        serve(g + 4 if e < last - 1 else g + 5)
        phase_two(e, g + 2)
        serve(g + 5 if e < last - 1 else g + 6)
    load_rows(last)
    for c in range(first_last, final, 2):
        serve(min(c + 5, final - 1))
        wait_far(c)
        wait_far(c + 1)
        low = units[c].low // FFB
        phase_one(last, low, low + units[c].size // FFB)
    serve(final)
    phase_two(last, final)

    for e in range(last):
        for step in range(dests - 1):
            j = dest_of(step)
            pltpu.make_async_remote_copy(
                src_ref=out_hbm.at[e, j], dst_ref=ret_hbm.at[e, j], send_sem=r_send.at[e, step], recv_sem=r_recv.at[e, j],
                device_id={'ep': j}, device_id_type=MESH).wait_recv()
    for n in range(fsdp):
        cols = pl.ds(n * d_shard, d_shard)
        for step in range(dests - 1):
            j = dest_of(step)
            pltpu.make_async_remote_copy(
                src_ref=out_hbm.at[last, j, :, cols], dst_ref=ret_hbm.at[last, j, :, cols], send_sem=c_send.at[n, step], recv_sem=c_recv.at[n, j],
                device_id={'ep': j}, device_id_type=MESH).wait_recv()
    for c in range(len(units)):
        for way in range(2):
            direct(c, way).wait_send()
            forward(c, way).wait_send()
    for step in range(dests - 1):
        for i in range(local):
            send_rows(i, step).wait_send()
        for e in range(last):
            back_rows(e, step).wait_send()
        for n in range(fsdp):
            back_cols(n, order[n], step).wait_send()


def exchange(per_expert, normed, w_gate, w_up, w_down, fsdp, dests, capacity):
    local, d_shard, ff = w_gate.shape
    tok_count, d_model = normed.shape
    units = unit_list(local, ff)
    rows = (local, dests, capacity, d_model)
    bf16 = jnp.bfloat16
    shapes = [rows, rows, rows, rows, (local, fsdp, d_shard, ff), (local, fsdp, d_shard, ff), (local, fsdp, ff, d_shard)]
    dma = pltpu.SemaphoreType.DMA
    anywhere = pl.BlockSpec(memory_space=pl.ANY)
    return pl.pallas_call(
        functools.partial(moe_kernel, units, capacity),
        out_shape=[jax.ShapeDtypeStruct(s, bf16) for s in shapes],
        in_specs=[pl.BlockSpec(memory_space=pltpu.VMEM)] + [anywhere] * 4,
        out_specs=[anywhere] * len(shapes),
        scratch_shapes=[
            pltpu.VMEM((tok_count, d_model), bf16),
            pltpu.VMEM((2, capacity, d_model), bf16),
            pltpu.VMEM((dests, capacity, d_model), bf16),
            pltpu.VMEM((dests * capacity, ff), bf16),
            pltpu.VMEM((2, 2, fsdp, d_shard, FFB), bf16),
            pltpu.VMEM((2, ff, d_shard), bf16),
            pltpu.VMEM((dests, capacity, d_shard), bf16),
            dma((len(units), 4)), dma((len(units), 4)),
            dma((local, dests)), dma((local, dests)),
            dma((local, dests)), dma((local, dests)),
            dma((fsdp, dests)), dma((fsdp, dests)),
            dma, dma((2,)), dma((dests,)), dma((2, 2, fsdp)), dma((2,)), dma((2,)),
        ],
        compiler_params=pltpu.CompilerParams(collective_id=0, has_side_effects=True, vmem_limit_bytes=VMEM_LIMIT),
        name='moe_exchange',
    )(per_expert, normed, w_gate, w_up, w_down)[0]


def local_block(hidden, norm_gain, w_router, w_gate, w_up, w_down, top2_ids, *, fsdp, dests):
    tok_local, d_model = hidden.shape
    num_experts = w_router.shape[1]
    local = w_gate.shape[0]
    capacity = (5 * tok_local + 2 * num_experts - 1) // (2 * num_experts)
    normed, gate_probs = norm_and_gates(hidden, norm_gain, w_router, top2_ids)
    slots, per_expert, starts = route(top2_ids, num_experts, capacity)
    tok = jnp.stack([slots[0].astype(jnp.float32), slots[1].astype(jnp.float32), gate_probs[:, 0], gate_probs[:, 1]], axis=1)
    ret = exchange(per_expert, normed, w_gate, w_up, w_down, fsdp, dests, capacity)
    return combine(hidden, [ret], list(range(local)), tok, starts, num_experts, capacity, local, jnp.bfloat16)


def solution(mesh):
    tok_spec = P(('dp', 'fsdp', 'ep'), None)
    in_specs = (tok_spec, P(None), P(None, None), P('ep', 'fsdp', None), P('ep', 'fsdp', None), P('ep', None, 'fsdp'), tok_spec)
    block = functools.partial(local_block, fsdp=mesh.shape['fsdp'], dests=mesh.shape['ep'])
    return jax.shard_map(block, mesh=mesh, in_specs=in_specs, out_specs=tok_spec, check_vma=False)
```

```python
import functools
from typing import NamedTuple

import jax
import jax.numpy as jnp
from jax import lax
from jax.experimental import pallas as pl
from jax.experimental.pallas import tpu as pltpu
from jax.sharding import PartitionSpec as P

EPS = 1e-5
TILE = 128
WIN = 32
SUB = 1
ALIGN = 8
ROUTE = 512
VMEM_LIMIT = 60 * 1024 * 1024


def window(starts_ref, tile, expert, round_idx, capacity):
    first = starts_ref[expert, tile] // ALIGN * ALIGN + round_idx * WIN
    base = jnp.minimum(first, capacity - WIN)
    return pl.multiple_of(base, ALIGN), first


def round_count(starts_ref, tile, experts, capacity):
    need = jnp.int32(0)
    for expert in experts:
        low = starts_ref[expert, tile] // ALIGN * ALIGN
        need = jnp.maximum(need, starts_ref[expert, tile + 1] - low)
    return (need + WIN - 1) // WIN


def combine_kernel(local, capacity, starts_ref, tok_ref, hidden_ref, ret_ref, out_ref, total):
    dests = ret_ref.shape[1]
    experts = [j * local + i for i in range(local) for j in range(dests)]
    width, lanes = len(experts) * WIN, 128
    spot = lax.broadcasted_iota(jnp.int32, (width // lanes, lanes), 0) * lanes + lax.broadcasted_iota(jnp.int32, (width // lanes, lanes), 1)
    which, inner = spot // WIN, spot % WIN

    def gathered(tile, tok, round_idx):
        slot = jnp.zeros(spot.shape, jnp.int32)
        valid = jnp.zeros(spot.shape, jnp.int32)
        rows = []
        for n, e in enumerate(experts):
            base, first = window(starts_ref, tile, e, round_idx, capacity)
            rows.append(ret_ref[e % local, e // local, pl.ds(base, WIN), :])
            slot = jnp.where(which == n, e * capacity + base, slot)
            valid = jnp.where(which == n, e * capacity + first, valid)
        slot = slot + inner
        slot = jnp.where(slot >= valid, slot, -2).astype(jnp.float32)
        picks = []
        for k in range(2):
            parts = [jnp.where(tok[:, k:k + 1] == slot[c:c + 1, :], 1.0, 0.0).astype(jnp.bfloat16) for c in range(width // lanes)]
            picks.append(jnp.concatenate(parts, axis=1))
        got = jnp.dot(jnp.concatenate(picks, axis=0), jnp.concatenate(rows, axis=0), preferred_element_type=jnp.float32)
        return tok[:, 2:3] * got[:TILE] + tok[:, 3:4] * got[TILE:]

    tiles = [pl.program_id(0) * SUB + n for n in range(SUB)]
    spans = [slice(n * TILE, (n + 1) * TILE) for n in range(SUB)]
    toks = [tok_ref[:, span].T for span in spans]
    for tile, span, tok in zip(tiles, spans, toks):
        out_ref[span, :] = (hidden_ref[span, :].astype(jnp.float32) + gathered(tile, tok, 0)).astype(out_ref.dtype)
    for tile, span, tok in zip(tiles, spans, toks):
        rounds = round_count(starts_ref, tile, experts, capacity)

        @pl.when(rounds > 1)
        def _():
            total[...] = hidden_ref[span, :].astype(jnp.float32)

            def more(round_idx, carry):
                total[...] += gathered(tile, tok, round_idx)
                return carry

            lax.fori_loop(0, rounds, more, 0)
            out_ref[span, :] = total[...].astype(out_ref.dtype)


def combine(hidden, ret, tok, starts, capacity):
    tok_count, d_model = hidden.shape
    local, dests = ret.shape[:2]
    return pl.pallas_call(
        functools.partial(combine_kernel, local, capacity),
        out_shape=jax.ShapeDtypeStruct(hidden.shape, hidden.dtype),
        grid_spec=pltpu.PrefetchScalarGridSpec(
            num_scalar_prefetch=1,
            grid=(tok_count // (TILE * SUB),),
            in_specs=[
                pl.BlockSpec((tok.shape[0], TILE * SUB), lambda t, s: (0, t)),
                pl.BlockSpec((TILE * SUB, d_model), lambda t, s: (t, 0)),
                pl.BlockSpec(ret.shape, lambda t, s: (0, 0, 0, 0), pipeline_mode=pl.Buffered(1)),
            ],
            out_specs=pl.BlockSpec((TILE * SUB, d_model), lambda t, s: (t, 0)),
            scratch_shapes=[pltpu.VMEM((TILE, d_model), jnp.float32)],
        ),
        compiler_params=pltpu.CompilerParams(dimension_semantics=('arbitrary',), vmem_limit_bytes=VMEM_LIMIT),
        cost_estimate=pl.CostEstimate(flops=4 * tok_count * local * dests * WIN * d_model, bytes_accessed=8 * tok_count * d_model, transcendentals=0),
        name='combine_rows',
    )(starts, tok, hidden, ret)


class Unit(NamedTuple):
    expert: int
    kind: int
    low: int
    size: int


GATE, UP, DOWN = 0, 1, 2
MESH = pl.DeviceIdType.MESH
AHEAD = 3
FFB = 256


def unit_list(local, ff):
    units = []
    cuts = [0, 1024, 2048, ff]
    for e in range(local):
        if e < local - 1:
            units += [Unit(e, GATE, 0, ff), Unit(e, UP, 0, ff)]
        else:
            for low, high in zip(cuts[:-1], cuts[1:]):
                units += [Unit(e, GATE, low, high - low), Unit(e, UP, low, high - low)]
        units.append(Unit(e, DOWN, 0, ff))
    return units


def moe_kernel(units, capacity, ids_ref, gain_ref, router_ref, hidden_hbm, gate_hbm, up_hbm, down_hbm,
               ret_hbm, tok_ref, starts_ref, send_hbm, recv_hbm, out_hbm, gate_all, up_all, down_all,
               normed, slots_ref, stage, rows, act, wbuf, dbuf, obuf,
               w_send, w_recv, a_send, a_recv, r_send, r_recv, c_send, c_recv,
               normed_sem, stage_sem, rows_sem, wbuf_sem, dbuf_sem, obuf_sem):
    local, d_shard, ff = gate_hbm.shape
    fsdp = gate_all.shape[1]
    dests = recv_hbm.shape[1]
    f_me, j_me = lax.axis_index('fsdp'), lax.axis_index('ep')
    right, left, far = lax.rem(f_me + 1, fsdp), lax.rem(f_me + fsdp - 1, fsdp), lax.rem(f_me + 2, fsdp)
    last = local - 1
    index = {(u.expert, u.kind, u.low): c for c, u in enumerate(units)}

    barrier = pltpu.get_barrier_semaphore()
    pl.semaphore_signal(barrier, inc=1, device_id={'fsdp': right}, device_id_type=MESH)
    pl.semaphore_signal(barrier, inc=1, device_id={'fsdp': left}, device_id_type=MESH)
    for step in range(1, dests):
        pl.semaphore_signal(barrier, inc=1, device_id={'ep': lax.rem(j_me + step, dests)}, device_id_type=MESH)
    pl.semaphore_wait(barrier, 2 + dests - 1)

    def own_part(u):
        if u.kind == DOWN:
            return down_hbm.at[u.expert]
        return (gate_hbm, up_hbm)[u.kind].at[u.expert, :, pl.ds(u.low, u.size)]

    def all_part(u, f, half=None):
        if u.kind == DOWN:
            span = pl.ds(0, ff) if half is None else pl.ds(half * (ff // 2), ff // 2)
            return down_all.at[u.expert, f, span, :]
        span = pl.ds(0, d_shard) if half is None else pl.ds(half * (d_shard // 2), d_shard // 2)
        return (gate_all, up_all)[u.kind].at[u.expert, f, span, pl.ds(u.low, u.size)]

    def direct(c, way):
        u = units[c]
        return pltpu.make_async_remote_copy(
            src_ref=own_part(u), dst_ref=all_part(u, f_me), send_sem=w_send.at[c, way], recv_sem=w_recv.at[c, way],
            device_id={'fsdp': (right, left)[way]}, device_id_type=MESH)

    def forward(c, way):
        u = units[c]
        part = all_part(u, (left, right)[way], way)
        return pltpu.make_async_remote_copy(
            src_ref=part, dst_ref=part, send_sem=w_send.at[c, 2 + way], recv_sem=w_recv.at[c, 2 + way],
            device_id={'fsdp': (right, left)[way]}, device_id_type=MESH)

    def start_direct(c):
        for way in range(2):
            direct(c, way).start()

    def service(c, then):
        for way in range(2):
            direct(c, way).wait_recv()
            forward(c, way).start()
        for n in then:
            start_direct(n)

    def wait_far(c):
        for way in range(2):
            forward(c, way).wait_recv()

    for c in range(AHEAD):
        start_direct(c)
    load = pltpu.make_async_copy(hidden_hbm, normed, normed_sem)
    load.start()
    load.wait()
    tok_count, d_model = normed.shape
    num_experts = local * dests
    gain = gain_ref[...].astype(jnp.float32)
    expert_iota = lax.broadcasted_iota(jnp.int32, (num_experts, ROUTE), 0)
    square = (ROUTE, ROUTE)
    earlier = jnp.where(lax.broadcasted_iota(jnp.int32, square, 0) < lax.broadcasted_iota(jnp.int32, square, 1), 1.0, 0.0).astype(jnp.bfloat16)
    tile_low = lax.broadcasted_iota(jnp.int32, (ROUTE, 128), 1) * TILE - lax.broadcasted_iota(jnp.int32, (ROUTE, 128), 0)

    def route(block, carry):
        seen, starts = carry
        low = pl.multiple_of(block * ROUTE, ROUTE)
        span = pl.ds(low, ROUTE)
        x = normed[span, :].astype(jnp.float32)
        mean_sq = jnp.mean(x * x, axis=-1, keepdims=True)
        u = (x * lax.rsqrt(mean_sq + EPS) * gain).astype(jnp.bfloat16)
        normed[span, :] = u
        logits = lax.dot_general(router_ref[...], u, (((1,), (1,)), ((), ())), preferred_element_type=jnp.float32)
        hits = [ids_ref[k:k + 1, span] == expert_iota for k in range(2)]
        chosen = jnp.where(hits[0] | hits[1], 1.0, 0.0)
        packed = chosen.astype(jnp.bfloat16)
        rank = jnp.dot(packed, earlier, preferred_element_type=jnp.float32) + seen
        keep = rank < capacity
        slots_ref[:, span] = jnp.where((chosen > 0) & keep, rank, -1.0).astype(jnp.int32)
        place = expert_iota.astype(jnp.float32) * capacity + rank + 1.0
        picked = []
        for k in range(2):
            tok_ref[k:k + 1, span] = jnp.sum(jnp.where(hits[k] & keep, place, 0.0), axis=0, keepdims=True) - 1.0
            picked.append(jnp.sum(jnp.where(hits[k], logits, 0.0), axis=0, keepdims=True))
        top = jnp.maximum(picked[0], picked[1])
        weights = [jnp.exp(p - top) for p in picked]
        for k in range(2):
            tok_ref[2 + k:3 + k, span] = weights[k] / (weights[0] + weights[1])
        tok_ref[4:8, span] = jnp.zeros((4, ROUTE), jnp.float32)
        before = jnp.where(tile_low > low, 1.0, 0.0).astype(jnp.bfloat16)
        starts = starts + jnp.dot(packed, before, preferred_element_type=jnp.float32)
        return seen + jnp.sum(chosen, axis=1, keepdims=True), starts

    zero = (jnp.zeros((num_experts, 1), jnp.float32), jnp.zeros((num_experts, 128), jnp.float32))
    _, starts = lax.fori_loop(0, tok_count // ROUTE, route, zero)
    starts_ref[...] = jnp.minimum(starts, capacity).astype(jnp.int32)

    def dest_of(step):
        return lax.rem(j_me + 1 + step, dests)

    def store_rows(i, step):
        slot = lax.rem(step, 2)
        return pltpu.make_async_copy(stage.at[slot], send_hbm.at[i, dest_of(step)], stage_sem.at[slot])

    def send_rows(i, step):
        j = dest_of(step)
        return pltpu.make_async_remote_copy(
            src_ref=send_hbm.at[i, j], dst_ref=recv_hbm.at[i, j_me], send_sem=a_send.at[i, step], recv_sem=a_recv.at[i, j_me],
            device_id={'ep': j}, device_id_type=MESH)

    row_iota = lax.broadcasted_iota(jnp.int32, (capacity, normed.shape[0]), 0)

    def dispatch(serve_at):
        def body(s, carry):
            i, step = s // dests, lax.rem(s, dests)
            want = slots_ref[pl.ds(dest_of(step) * local + i, 1), :]
            pick = jnp.where(row_iota == want, 1.0, 0.0).astype(jnp.bfloat16)
            stage[lax.rem(s, 2)] = jnp.dot(pick, normed[...], preferred_element_type=jnp.float32).astype(jnp.bfloat16)

            @pl.when(step > 0)
            def _():
                store_rows(i, step - 1).wait()
                send_rows(i, step - 1).start()

            store_rows(i, step).start()

            @pl.when(step == dests - 1)
            def _():
                store_rows(i, step).wait()

            for at, act_on in serve_at.items():
                pl.when(s == at)(act_on)
            return carry

        lax.fori_loop(0, local * dests, body, 0)

    def load_rows(e):
        def copy(step):
            j = dest_of(step)
            if step == dests - 1:
                return pltpu.make_async_copy(send_hbm.at[e, j], rows.at[j], rows_sem.at[step])
            return pltpu.make_async_copy(recv_hbm.at[e, j], rows.at[j], rows_sem.at[step])

        for step in range(dests - 1):
            j = dest_of(step)
            pltpu.make_async_remote_copy(
                src_ref=send_hbm.at[e, j], dst_ref=recv_hbm.at[e, j], send_sem=a_send.at[e, step], recv_sem=a_recv.at[e, j],
                device_id={'ep': j}, device_id_type=MESH).wait_recv()
        for step in range(dests):
            copy(step).start()
        for step in range(dests):
            copy(step).wait()

    def block_copies(e, b, slot):
        cols = pl.ds(pl.multiple_of(b * FFB, FFB), FFB)
        copies = []
        for m, (own, whole) in enumerate(((gate_hbm, gate_all), (up_hbm, up_all))):
            for r in range(fsdp):
                f = lax.rem(f_me + r, fsdp)
                src = own.at[e, :, cols] if r == 0 else whole.at[e, f, :, cols]
                copies.append(pltpu.make_async_copy(src, wbuf.at[slot, m, f], wbuf_sem.at[slot, m, r]))
        return copies

    def phase_one(e, low, high):
        for copy in block_copies(e, low, low % 2):
            copy.start()

        def body(b, carry):
            slot = lax.rem(b, 2)

            @pl.when(b + 1 < high)
            def _():
                for copy in block_copies(e, b + 1, 1 - slot):
                    copy.start()

            for copy in block_copies(e, b, slot):
                copy.wait()
            gate = wbuf[slot, GATE].reshape(fsdp * d_shard, FFB)
            up = wbuf[slot, UP].reshape(fsdp * d_shard, FFB)
            for r in range(dests // 2):
                x = rows[2 * r:2 * r + 2].reshape(2 * capacity, fsdp * d_shard)
                a = jnp.dot(x, gate, preferred_element_type=jnp.float32)
                u = jnp.dot(x, up, preferred_element_type=jnp.float32)
                act[2 * r * capacity:(2 * r + 2) * capacity, pl.ds(pl.multiple_of(b * FFB, FFB), FFB)] = (a * jax.nn.sigmoid(a) * u).astype(jnp.bfloat16)
            return carry

        lax.fori_loop(low, high, body, 0)

    def back_rows(e, step):
        j = dest_of(step)
        return pltpu.make_async_remote_copy(
            src_ref=out_hbm.at[e, j], dst_ref=ret_hbm.at[e, j_me], send_sem=r_send.at[e, step], recv_sem=r_recv.at[e, j_me],
            device_id={'ep': j}, device_id_type=MESH)

    def back_cols(n, f, step):
        j = dest_of(step)
        cols = pl.ds(pl.multiple_of(f * d_shard, d_shard), d_shard)
        return pltpu.make_async_remote_copy(
            src_ref=out_hbm.at[last, j, :, cols], dst_ref=ret_hbm.at[last, j_me, :, cols], send_sem=c_send.at[n, step], recv_sem=c_recv.at[f, j_me],
            device_id={'ep': j}, device_id_type=MESH)

    order = (f_me, left, right, far)

    def down_load(e, n):
        src = down_hbm.at[e] if n == 0 else down_all.at[e, order[n]]
        return pltpu.make_async_copy(src, dbuf.at[n % 2], dbuf_sem.at[n % 2])

    def down_column(e, n):
        f = order[n]

        def body(r, carry):
            hid = act[pl.ds(pl.multiple_of(r * 2 * capacity, 2 * capacity), 2 * capacity), :]
            got = jnp.dot(hid, dbuf[n % 2], preferred_element_type=jnp.float32).astype(jnp.bfloat16)
            obuf[pl.ds(2 * r, 2)] = got.reshape(2, capacity, d_shard)
            return carry

        lax.fori_loop(0, dests // 2, body, 0)
        cols = pl.ds(pl.multiple_of(f * d_shard, d_shard), d_shard)
        mine = pltpu.make_async_copy(obuf.at[j_me], ret_hbm.at[e, j_me, :, cols], obuf_sem.at[0])
        rest = pltpu.make_async_copy(obuf, out_hbm.at[e, :, :, cols], obuf_sem.at[1])
        mine.start()
        rest.start()
        mine.wait()
        rest.wait()

    def phase_two(e, far_unit):
        down_load(e, 0).start()
        if e < last:
            down_load(e, 1).start()
        down_load(e, 0).wait()
        down_column(e, 0)
        if e == last:
            for step in range(dests - 1):
                back_cols(0, order[0], step).start()
            serve(far_unit)
            down_load(e, 1).start()
        down_load(e, 2).start()
        down_load(e, 1).wait()
        down_column(e, 1)
        if e == last:
            for step in range(dests - 1):
                back_cols(1, order[1], step).start()
        down_load(e, 2).wait()
        down_column(e, 2)
        if e == last:
            for step in range(dests - 1):
                back_cols(2, order[2], step).start()
        wait_far(far_unit)
        down_load(e, 3).start()
        down_load(e, 3).wait()
        down_column(e, 3)
        for step in range(dests - 1):
            if e == last:
                back_cols(3, order[3], step).start()
            else:
                back_rows(e, step).start()

    first_last = index[last, GATE, 0]
    final = index[last, DOWN, 0]

    def then(c):
        n = c + AHEAD
        if n < final:
            return (n,)
        return (final,) if c == final - 1 else ()

    done = 0

    def serve(upto):
        nonlocal done
        while done <= upto:
            service(done, then(done))
            done += 1

    dispatch({(i + 1) * dests - 1: functools.partial(serve, i) for i in range(local - 1)})
    blocks = ff // FFB
    for e in range(last):
        g = index[e, GATE, 0]
        serve(g + 3)
        wait_far(g)
        wait_far(g + 1)
        load_rows(e)
        phase_one(e, 0, blocks)
        serve(g + 4 if e < last - 1 else g + 5)
        phase_two(e, g + 2)
        serve(g + 5 if e < last - 1 else g + 6)
    load_rows(last)
    for c in range(first_last, final, 2):
        serve(min(c + 5, final - 1))
        wait_far(c)
        wait_far(c + 1)
        low = units[c].low // FFB
        phase_one(last, low, low + units[c].size // FFB)
    phase_two(last, final)

    for e in range(last):
        for step in range(dests - 1):
            j = dest_of(step)
            pltpu.make_async_remote_copy(
                src_ref=out_hbm.at[e, j], dst_ref=ret_hbm.at[e, j], send_sem=r_send.at[e, step], recv_sem=r_recv.at[e, j],
                device_id={'ep': j}, device_id_type=MESH).wait_recv()
    for n in range(fsdp):
        cols = pl.ds(n * d_shard, d_shard)
        for step in range(dests - 1):
            j = dest_of(step)
            pltpu.make_async_remote_copy(
                src_ref=out_hbm.at[last, j, :, cols], dst_ref=ret_hbm.at[last, j, :, cols], send_sem=c_send.at[n, step], recv_sem=c_recv.at[n, j],
                device_id={'ep': j}, device_id_type=MESH).wait_recv()
    for c in range(len(units)):
        for way in range(2):
            direct(c, way).wait_send()
            forward(c, way).wait_send()
    for step in range(dests - 1):
        for i in range(local):
            send_rows(i, step).wait_send()
        for e in range(last):
            back_rows(e, step).wait_send()
        for n in range(fsdp):
            back_cols(n, order[n], step).wait_send()


def exchange(top2_ids, norm_gain, w_router, hidden, w_gate, w_up, w_down, fsdp, dests, capacity):
    local, d_shard, ff = w_gate.shape
    tok_count, d_model = hidden.shape
    num_experts = w_router.shape[1]
    units = unit_list(local, ff)
    rows = (local, dests, capacity, d_model)
    bf16 = jnp.bfloat16
    shapes = [rows, rows, rows, (local, fsdp, d_shard, ff), (local, fsdp, d_shard, ff), (local, fsdp, ff, d_shard)]
    dma = pltpu.SemaphoreType.DMA
    anywhere = pl.BlockSpec(memory_space=pl.ANY)
    vmem = pl.BlockSpec(memory_space=pltpu.VMEM)
    return pl.pallas_call(
        functools.partial(moe_kernel, units, capacity),
        out_shape=[jax.ShapeDtypeStruct(rows, bf16), jax.ShapeDtypeStruct((8, tok_count), jnp.float32), jax.ShapeDtypeStruct((num_experts, 128), jnp.int32)]
        + [jax.ShapeDtypeStruct(s, bf16) for s in shapes],
        in_specs=[vmem] * 3 + [anywhere] * 4,
        out_specs=[anywhere, vmem, vmem] + [anywhere] * len(shapes),
        scratch_shapes=[
            pltpu.VMEM((tok_count, d_model), bf16),
            pltpu.VMEM((num_experts, tok_count), jnp.int32),
            pltpu.VMEM((2, capacity, d_model), bf16),
            pltpu.VMEM((dests, capacity, d_model), bf16),
            pltpu.VMEM((dests * capacity, ff), bf16),
            pltpu.VMEM((2, 2, fsdp, d_shard, FFB), bf16),
            pltpu.VMEM((2, ff, d_shard), bf16),
            pltpu.VMEM((dests, capacity, d_shard), bf16),
            dma((len(units), 4)), dma((len(units), 4)),
            dma((local, dests)), dma((local, dests)),
            dma((local, dests)), dma((local, dests)),
            dma((fsdp, dests)), dma((fsdp, dests)),
            dma, dma((2,)), dma((dests,)), dma((2, 2, fsdp)), dma((2,)), dma((2,)),
        ],
        compiler_params=pltpu.CompilerParams(collective_id=0, has_side_effects=True, vmem_limit_bytes=VMEM_LIMIT),
        name='moe_exchange',
    )(top2_ids.T, norm_gain.reshape(1, d_model), w_router.T, hidden, w_gate, w_up, w_down)[:3]


def local_block(hidden, norm_gain, w_router, w_gate, w_up, w_down, top2_ids, *, fsdp, dests):
    tok_local = hidden.shape[0]
    num_experts = w_router.shape[1]
    capacity = (5 * tok_local + 2 * num_experts - 1) // (2 * num_experts)
    ret, tok, starts = exchange(top2_ids, norm_gain, w_router, hidden, w_gate, w_up, w_down, fsdp, dests, capacity)
    return combine(hidden, ret, tok, starts, capacity)


def solution(mesh):
    tok_spec = P(('dp', 'fsdp', 'ep'), None)
    in_specs = (tok_spec, P(None), P(None, None), P('ep', 'fsdp', None), P('ep', 'fsdp', None), P('ep', None, 'fsdp'), tok_spec)
    block = functools.partial(local_block, fsdp=mesh.shape['fsdp'], dests=mesh.shape['ep'])
    return jax.shard_map(block, mesh=mesh, in_specs=in_specs, out_specs=tok_spec, check_vma=False)
```

```python
import functools
from typing import NamedTuple

import jax
import jax.numpy as jnp
from jax import lax
from jax.experimental import pallas as pl
from jax.experimental.pallas import tpu as pltpu
from jax.sharding import PartitionSpec as P

EPS = 1e-5
TILE = 128
WIN = 32
SUB = 2
ALIGN = 8
ROUTE = 512
VMEM_LIMIT = 60 * 1024 * 1024


ROUNDS, FIRSTS = 32, 40


def combine_kernel(local, capacity, plan_ref, tok_ref, slot_ref, hidden_ref, ret_ref, out_ref, total):
    dests = ret_ref.shape[1]
    experts = [j * local + i for i in range(local) for j in range(dests)]
    width, lanes = len(experts) * WIN, 128

    def picked(tok, slots, rows):
        picks = []
        for k in range(2):
            parts = [jnp.where(tok[:, k:k + 1] == slots[c], 1.0, 0.0).astype(jnp.bfloat16) for c in range(width // lanes)]
            picks.append(jnp.concatenate(parts, axis=1))
        got = jnp.dot(jnp.concatenate(picks, axis=0), jnp.concatenate(rows, axis=0), preferred_element_type=jnp.float32)
        return tok[:, 2:3] * got[:TILE] + tok[:, 3:4] * got[TILE:]

    tiles = [pl.program_id(0) * SUB + n for n in range(SUB)]
    spans = [slice(n * TILE, (n + 1) * TILE) for n in range(SUB)]
    toks = [tok_ref[:, span].T for span in spans]
    for tile, span, tok in zip(tiles, spans, toks):
        rows = [ret_ref[e % local, e // local, pl.ds(pl.multiple_of(plan_ref[tile, e], ALIGN), WIN), :] for e in experts]
        line = slot_ref[pl.ds(lax.rem(tile, 8), 1), :]
        slots = [line[:, c * lanes:(c + 1) * lanes] for c in range(width // lanes)]
        out_ref[span, :] = (hidden_ref[span, :].astype(jnp.float32) + picked(tok, slots, rows)).astype(out_ref.dtype)

    spot = lax.broadcasted_iota(jnp.int32, (width // lanes, lanes), 0) * lanes + lax.broadcasted_iota(jnp.int32, (width // lanes, lanes), 1)
    which, inner = spot // WIN, spot % WIN
    for tile, span, tok in zip(tiles, spans, toks):
        rounds = plan_ref[tile, ROUNDS]

        @pl.when(rounds > 1)
        def _():
            total[...] = hidden_ref[span, :].astype(jnp.float32)

            def more(round_idx, carry):
                slot = jnp.zeros(spot.shape, jnp.int32)
                valid = jnp.zeros(spot.shape, jnp.int32)
                rows = []
                for n, e in enumerate(experts):
                    first = plan_ref[tile, FIRSTS + e] + round_idx * WIN
                    base = pl.multiple_of(jnp.minimum(first, capacity - WIN), ALIGN)
                    rows.append(ret_ref[e % local, e // local, pl.ds(base, WIN), :])
                    slot = jnp.where(which == n, e * capacity + base, slot)
                    valid = jnp.where(which == n, e * capacity + first, valid)
                slot = slot + inner
                slot = jnp.where(slot >= valid, slot, -2).astype(jnp.float32)
                total[...] += picked(tok, [slot[c:c + 1, :] for c in range(width // lanes)], rows)
                return carry

            lax.fori_loop(0, rounds, more, 0)
            out_ref[span, :] = total[...].astype(out_ref.dtype)


def combine(hidden, ret, tok, plan, slots, capacity):
    tok_count, d_model = hidden.shape
    local, dests = ret.shape[:2]
    step = TILE * SUB
    return pl.pallas_call(
        functools.partial(combine_kernel, local, capacity),
        out_shape=jax.ShapeDtypeStruct(hidden.shape, hidden.dtype),
        grid_spec=pltpu.PrefetchScalarGridSpec(
            num_scalar_prefetch=1,
            grid=(tok_count // step,),
            in_specs=[
                pl.BlockSpec((tok.shape[0], step), lambda t, s: (0, t)),
                pl.BlockSpec((8, slots.shape[1]), lambda t, s: (t * SUB // 8, 0)),
                pl.BlockSpec((step, d_model), lambda t, s: (t, 0)),
                pl.BlockSpec(ret.shape, lambda t, s: (0, 0, 0, 0), pipeline_mode=pl.Buffered(1)),
            ],
            out_specs=pl.BlockSpec((step, d_model), lambda t, s: (t, 0)),
            scratch_shapes=[pltpu.VMEM((TILE, d_model), jnp.float32)],
        ),
        compiler_params=pltpu.CompilerParams(dimension_semantics=('arbitrary',), vmem_limit_bytes=VMEM_LIMIT),
        cost_estimate=pl.CostEstimate(flops=4 * tok_count * local * dests * WIN * d_model, bytes_accessed=8 * tok_count * d_model, transcendentals=0),
        name='combine_rows',
    )(plan, tok, slots, hidden, ret)


class Unit(NamedTuple):
    expert: int
    kind: int
    low: int
    size: int


GATE, UP, DOWN = 0, 1, 2
MESH = pl.DeviceIdType.MESH
AHEAD = 3
FFB = 256


def unit_list(local, ff):
    units = []
    cuts = [0, 1024, 2048, ff]
    for e in range(local):
        if e < local - 1:
            units += [Unit(e, GATE, 0, ff), Unit(e, UP, 0, ff)]
        else:
            for low, high in zip(cuts[:-1], cuts[1:]):
                units += [Unit(e, GATE, low, high - low), Unit(e, UP, low, high - low)]
        units.append(Unit(e, DOWN, 0, ff))
    return units


def moe_kernel(units, capacity, ids_ref, gain_ref, router_ref, hidden_hbm, gate_hbm, up_hbm, down_hbm,
               ret_hbm, tok_ref, plan_ref, line_ref, send_hbm, recv_hbm, out_hbm, gate_all, up_all, down_all,
               normed, slots_ref, stage, rows, act, wbuf, dbuf, obuf,
               w_send, w_recv, a_send, a_recv, r_send, r_recv, c_send, c_recv,
               normed_sem, stage_sem, rows_sem, wbuf_sem, dbuf_sem, obuf_sem):
    local, d_shard, ff = gate_hbm.shape
    fsdp = gate_all.shape[1]
    dests = recv_hbm.shape[1]
    f_me, j_me = lax.axis_index('fsdp'), lax.axis_index('ep')
    right, left, far = lax.rem(f_me + 1, fsdp), lax.rem(f_me + fsdp - 1, fsdp), lax.rem(f_me + 2, fsdp)
    last = local - 1
    index = {(u.expert, u.kind, u.low): c for c, u in enumerate(units)}

    barrier = pltpu.get_barrier_semaphore()
    pl.semaphore_signal(barrier, inc=1, device_id={'fsdp': right}, device_id_type=MESH)
    pl.semaphore_signal(barrier, inc=1, device_id={'fsdp': left}, device_id_type=MESH)
    for step in range(1, dests):
        pl.semaphore_signal(barrier, inc=1, device_id={'ep': lax.rem(j_me + step, dests)}, device_id_type=MESH)
    pl.semaphore_wait(barrier, 2 + dests - 1)

    def own_part(u):
        if u.kind == DOWN:
            return down_hbm.at[u.expert]
        return (gate_hbm, up_hbm)[u.kind].at[u.expert, :, pl.ds(u.low, u.size)]

    def all_part(u, f, half=None):
        if u.kind == DOWN:
            span = pl.ds(0, ff) if half is None else pl.ds(half * (ff // 2), ff // 2)
            return down_all.at[u.expert, f, span, :]
        span = pl.ds(0, d_shard) if half is None else pl.ds(half * (d_shard // 2), d_shard // 2)
        return (gate_all, up_all)[u.kind].at[u.expert, f, span, pl.ds(u.low, u.size)]

    def direct(c, way):
        u = units[c]
        return pltpu.make_async_remote_copy(
            src_ref=own_part(u), dst_ref=all_part(u, f_me), send_sem=w_send.at[c, way], recv_sem=w_recv.at[c, way],
            device_id={'fsdp': (right, left)[way]}, device_id_type=MESH)

    def forward(c, way):
        u = units[c]
        part = all_part(u, (left, right)[way], way)
        return pltpu.make_async_remote_copy(
            src_ref=part, dst_ref=part, send_sem=w_send.at[c, 2 + way], recv_sem=w_recv.at[c, 2 + way],
            device_id={'fsdp': (right, left)[way]}, device_id_type=MESH)

    def start_direct(c):
        for way in range(2):
            direct(c, way).start()

    def service(c, then):
        for way in range(2):
            direct(c, way).wait_recv()
            forward(c, way).start()
        for n in then:
            start_direct(n)

    def wait_far(c):
        for way in range(2):
            forward(c, way).wait_recv()

    for c in range(AHEAD):
        start_direct(c)
    load = pltpu.make_async_copy(hidden_hbm, normed, normed_sem)
    load.start()
    load.wait()
    tok_count, d_model = normed.shape
    num_experts = local * dests
    gain = gain_ref[...].astype(jnp.float32)
    expert_iota = lax.broadcasted_iota(jnp.int32, (num_experts, ROUTE), 0)
    square = (ROUTE, ROUTE)
    earlier = jnp.where(lax.broadcasted_iota(jnp.int32, square, 0) < lax.broadcasted_iota(jnp.int32, square, 1), 1.0, 0.0).astype(jnp.bfloat16)
    tile_low = lax.broadcasted_iota(jnp.int32, (ROUTE, 128), 1) * TILE - lax.broadcasted_iota(jnp.int32, (ROUTE, 128), 0)

    def route(block, carry):
        seen, starts, ends = carry
        low = pl.multiple_of(block * ROUTE, ROUTE)
        span = pl.ds(low, ROUTE)
        x = normed[span, :].astype(jnp.float32)
        mean_sq = jnp.mean(x * x, axis=-1, keepdims=True)
        u = (x * lax.rsqrt(mean_sq + EPS) * gain).astype(jnp.bfloat16)
        normed[span, :] = u
        logits = lax.dot_general(router_ref[...], u, (((1,), (1,)), ((), ())), preferred_element_type=jnp.float32)
        hits = [ids_ref[k:k + 1, span] == expert_iota for k in range(2)]
        chosen = jnp.where(hits[0] | hits[1], 1.0, 0.0)
        packed = chosen.astype(jnp.bfloat16)
        rank = jnp.dot(packed, earlier, preferred_element_type=jnp.float32) + seen
        keep = rank < capacity
        slots_ref[:, span] = jnp.where((chosen > 0) & keep, rank, -1.0).astype(jnp.int32)
        place = expert_iota.astype(jnp.float32) * capacity + rank + 1.0
        picked = []
        for k in range(2):
            tok_ref[k:k + 1, span] = jnp.sum(jnp.where(hits[k] & keep, place, 0.0), axis=0, keepdims=True) - 1.0
            picked.append(jnp.sum(jnp.where(hits[k], logits, 0.0), axis=0, keepdims=True))
        top = jnp.maximum(picked[0], picked[1])
        weights = [jnp.exp(p - top) for p in picked]
        for k in range(2):
            tok_ref[2 + k:3 + k, span] = weights[k] / (weights[0] + weights[1])
        tok_ref[4:8, span] = jnp.zeros((4, ROUTE), jnp.float32)
        before = [jnp.where(tile_low + n * TILE > low, 1.0, 0.0).astype(jnp.bfloat16) for n in range(2)]
        starts = starts + jnp.dot(packed, before[0], preferred_element_type=jnp.float32)
        ends = ends + jnp.dot(packed, before[1], preferred_element_type=jnp.float32)
        return seen + jnp.sum(chosen, axis=1, keepdims=True), starts, ends

    counts = jnp.zeros((num_experts, 128), jnp.float32)
    _, starts, ends = lax.fori_loop(0, tok_count // ROUTE, route, (jnp.zeros((num_experts, 1), jnp.float32), counts, counts))
    eighths = jnp.minimum(starts, capacity).astype(jnp.int32) // ALIGN
    bases = jnp.minimum(eighths, (capacity - WIN) // ALIGN)
    need = jnp.max(jnp.minimum(ends, capacity).astype(jnp.int32) - eighths * ALIGN, axis=0, keepdims=True)
    rounds = jnp.broadcast_to((need + WIN - 1) // WIN, (8, 128))
    blank = jnp.zeros((128 - 8 - 2 * num_experts, 128), jnp.int32)
    plan = jnp.concatenate([bases * ALIGN, rounds, eighths * ALIGN, blank], axis=0).astype(jnp.float32).T
    tiles, width = line_ref.shape
    plan_ref[...] = plan[:tiles].astype(jnp.int32)
    spot = lax.broadcasted_iota(jnp.int32, (128, width), 1)
    source = lax.broadcasted_iota(jnp.int32, (128, width), 0)
    which = spot // WIN
    owner = lax.rem(which, dests) * local + which // dests
    spread = [jnp.where(source == owner + n * FIRSTS, 1.0, 0.0).astype(jnp.bfloat16) for n in range(2)]
    scaled = (plan[:tiles] * (1.0 / ALIGN)).astype(jnp.bfloat16)
    base, first = [jnp.dot(scaled, m, preferred_element_type=jnp.float32) * ALIGN for m in spread]
    inner = (spot - which * WIN)[:tiles].astype(jnp.float32)
    line_ref[...] = jnp.where(base + inner >= first, owner[:tiles].astype(jnp.float32) * capacity + base + inner, -2.0)

    def dest_of(step):
        return lax.rem(j_me + 1 + step, dests)

    def store_rows(i, step):
        slot = lax.rem(step, 2)
        return pltpu.make_async_copy(stage.at[slot], send_hbm.at[i, dest_of(step)], stage_sem.at[slot])

    def send_rows(i, step):
        j = dest_of(step)
        return pltpu.make_async_remote_copy(
            src_ref=send_hbm.at[i, j], dst_ref=recv_hbm.at[i, j_me], send_sem=a_send.at[i, step], recv_sem=a_recv.at[i, j_me],
            device_id={'ep': j}, device_id_type=MESH)

    row_iota = lax.broadcasted_iota(jnp.int32, (capacity, normed.shape[0]), 0)

    def dispatch(serve_at):
        def body(s, carry):
            i, step = s // dests, lax.rem(s, dests)
            want = slots_ref[pl.ds(dest_of(step) * local + i, 1), :]
            pick = jnp.where(row_iota == want, 1.0, 0.0).astype(jnp.bfloat16)
            stage[lax.rem(s, 2)] = jnp.dot(pick, normed[...], preferred_element_type=jnp.float32).astype(jnp.bfloat16)

            @pl.when(step > 0)
            def _():
                store_rows(i, step - 1).wait()
                send_rows(i, step - 1).start()

            store_rows(i, step).start()

            @pl.when(step == dests - 1)
            def _():
                store_rows(i, step).wait()

            for at, act_on in serve_at.items():
                pl.when(s == at)(act_on)
            return carry

        lax.fori_loop(0, local * dests, body, 0)

    def load_rows(e):
        def copy(step):
            j = dest_of(step)
            if step == dests - 1:
                return pltpu.make_async_copy(send_hbm.at[e, j], rows.at[j], rows_sem.at[step])
            return pltpu.make_async_copy(recv_hbm.at[e, j], rows.at[j], rows_sem.at[step])

        for step in range(dests - 1):
            j = dest_of(step)
            pltpu.make_async_remote_copy(
                src_ref=send_hbm.at[e, j], dst_ref=recv_hbm.at[e, j], send_sem=a_send.at[e, step], recv_sem=a_recv.at[e, j],
                device_id={'ep': j}, device_id_type=MESH).wait_recv()
        for step in range(dests):
            copy(step).start()
        for step in range(dests):
            copy(step).wait()

    def block_copies(e, b, slot):
        cols = pl.ds(pl.multiple_of(b * FFB, FFB), FFB)
        copies = []
        for m, (own, whole) in enumerate(((gate_hbm, gate_all), (up_hbm, up_all))):
            for r in range(fsdp):
                f = lax.rem(f_me + r, fsdp)
                src = own.at[e, :, cols] if r == 0 else whole.at[e, f, :, cols]
                copies.append(pltpu.make_async_copy(src, wbuf.at[slot, m, f], wbuf_sem.at[slot, m, r]))
        return copies

    def phase_one(e, low, high):
        for copy in block_copies(e, low, low % 2):
            copy.start()

        def body(b, carry):
            slot = lax.rem(b, 2)

            @pl.when(b + 1 < high)
            def _():
                for copy in block_copies(e, b + 1, 1 - slot):
                    copy.start()

            for copy in block_copies(e, b, slot):
                copy.wait()
            gate = wbuf[slot, GATE].reshape(fsdp * d_shard, FFB)
            up = wbuf[slot, UP].reshape(fsdp * d_shard, FFB)
            for r in range(dests // 2):
                x = rows[2 * r:2 * r + 2].reshape(2 * capacity, fsdp * d_shard)
                a = jnp.dot(x, gate, preferred_element_type=jnp.float32)
                u = jnp.dot(x, up, preferred_element_type=jnp.float32)
                act[2 * r * capacity:(2 * r + 2) * capacity, pl.ds(pl.multiple_of(b * FFB, FFB), FFB)] = (a * jax.nn.sigmoid(a) * u).astype(jnp.bfloat16)
            return carry

        lax.fori_loop(low, high, body, 0)

    def back_rows(e, step):
        j = dest_of(step)
        return pltpu.make_async_remote_copy(
            src_ref=out_hbm.at[e, j], dst_ref=ret_hbm.at[e, j_me], send_sem=r_send.at[e, step], recv_sem=r_recv.at[e, j_me],
            device_id={'ep': j}, device_id_type=MESH)

    def back_cols(n, f, step):
        j = dest_of(step)
        cols = pl.ds(pl.multiple_of(f * d_shard, d_shard), d_shard)
        return pltpu.make_async_remote_copy(
            src_ref=out_hbm.at[last, j, :, cols], dst_ref=ret_hbm.at[last, j_me, :, cols], send_sem=c_send.at[n, step], recv_sem=c_recv.at[f, j_me],
            device_id={'ep': j}, device_id_type=MESH)

    order = (f_me, left, right, far)

    def down_load(e, n):
        src = down_hbm.at[e] if n == 0 else down_all.at[e, order[n]]
        return pltpu.make_async_copy(src, dbuf.at[n % 2], dbuf_sem.at[n % 2])

    def down_column(e, n):
        f = order[n]

        def body(r, carry):
            hid = act[pl.ds(pl.multiple_of(r * 2 * capacity, 2 * capacity), 2 * capacity), :]
            got = jnp.dot(hid, dbuf[n % 2], preferred_element_type=jnp.float32).astype(jnp.bfloat16)
            obuf[pl.ds(2 * r, 2)] = got.reshape(2, capacity, d_shard)
            return carry

        lax.fori_loop(0, dests // 2, body, 0)
        cols = pl.ds(pl.multiple_of(f * d_shard, d_shard), d_shard)
        mine = pltpu.make_async_copy(obuf.at[j_me], ret_hbm.at[e, j_me, :, cols], obuf_sem.at[0])
        rest = pltpu.make_async_copy(obuf, out_hbm.at[e, :, :, cols], obuf_sem.at[1])
        mine.start()
        rest.start()
        mine.wait()
        rest.wait()

    def phase_two(e, far_unit):
        down_load(e, 0).start()
        if e < last:
            down_load(e, 1).start()
        down_load(e, 0).wait()
        down_column(e, 0)
        if e == last:
            for step in range(dests - 1):
                back_cols(0, order[0], step).start()
            serve(far_unit)
            down_load(e, 1).start()
        down_load(e, 2).start()
        down_load(e, 1).wait()
        down_column(e, 1)
        if e == last:
            for step in range(dests - 1):
                back_cols(1, order[1], step).start()
        down_load(e, 2).wait()
        down_column(e, 2)
        if e == last:
            for step in range(dests - 1):
                back_cols(2, order[2], step).start()
        wait_far(far_unit)
        down_load(e, 3).start()
        down_load(e, 3).wait()
        down_column(e, 3)
        for step in range(dests - 1):
            if e == last:
                back_cols(3, order[3], step).start()
            else:
                back_rows(e, step).start()

    first_last = index[last, GATE, 0]
    final = index[last, DOWN, 0]

    def then(c):
        n = c + AHEAD
        if n < final:
            return (n,)
        return (final,) if c == final - 1 else ()

    done = 0

    def serve(upto):
        nonlocal done
        while done <= upto:
            service(done, then(done))
            done += 1

    dispatch({(i + 1) * dests - 1: functools.partial(serve, i) for i in range(local - 1)})
    blocks = ff // FFB
    for e in range(last):
        g = index[e, GATE, 0]
        serve(g + 3)
        wait_far(g)
        wait_far(g + 1)
        load_rows(e)
        phase_one(e, 0, blocks)
        serve(g + 4 if e < last - 1 else g + 5)
        phase_two(e, g + 2)
        serve(g + 5 if e < last - 1 else g + 6)
    load_rows(last)
    for c in range(first_last, final, 2):
        serve(min(c + 5, final - 1))
        wait_far(c)
        wait_far(c + 1)
        low = units[c].low // FFB
        phase_one(last, low, low + units[c].size // FFB)
    phase_two(last, final)

    for e in range(last):
        for step in range(dests - 1):
            j = dest_of(step)
            pltpu.make_async_remote_copy(
                src_ref=out_hbm.at[e, j], dst_ref=ret_hbm.at[e, j], send_sem=r_send.at[e, step], recv_sem=r_recv.at[e, j],
                device_id={'ep': j}, device_id_type=MESH).wait_recv()
    for n in range(fsdp):
        cols = pl.ds(n * d_shard, d_shard)
        for step in range(dests - 1):
            j = dest_of(step)
            pltpu.make_async_remote_copy(
                src_ref=out_hbm.at[last, j, :, cols], dst_ref=ret_hbm.at[last, j, :, cols], send_sem=c_send.at[n, step], recv_sem=c_recv.at[n, j],
                device_id={'ep': j}, device_id_type=MESH).wait_recv()
    for c in range(len(units)):
        for way in range(2):
            direct(c, way).wait_send()
            forward(c, way).wait_send()
    for step in range(dests - 1):
        for i in range(local):
            send_rows(i, step).wait_send()
        for e in range(last):
            back_rows(e, step).wait_send()
        for n in range(fsdp):
            back_cols(n, order[n], step).wait_send()


def exchange(top2_ids, norm_gain, w_router, hidden, w_gate, w_up, w_down, fsdp, dests, capacity):
    local, d_shard, ff = w_gate.shape
    tok_count, d_model = hidden.shape
    num_experts = w_router.shape[1]
    units = unit_list(local, ff)
    rows = (local, dests, capacity, d_model)
    bf16 = jnp.bfloat16
    shapes = [rows, rows, rows, (local, fsdp, d_shard, ff), (local, fsdp, d_shard, ff), (local, fsdp, ff, d_shard)]
    dma = pltpu.SemaphoreType.DMA
    anywhere = pl.BlockSpec(memory_space=pl.ANY)
    vmem = pl.BlockSpec(memory_space=pltpu.VMEM)
    return pl.pallas_call(
        functools.partial(moe_kernel, units, capacity),
        out_shape=[jax.ShapeDtypeStruct(rows, bf16), jax.ShapeDtypeStruct((8, tok_count), jnp.float32), jax.ShapeDtypeStruct((tok_count // TILE, 128), jnp.int32), jax.ShapeDtypeStruct((tok_count // TILE, num_experts * WIN), jnp.float32)]
        + [jax.ShapeDtypeStruct(s, bf16) for s in shapes],
        in_specs=[vmem] * 3 + [anywhere] * 4,
        out_specs=[anywhere, vmem, vmem, vmem] + [anywhere] * len(shapes),
        scratch_shapes=[
            pltpu.VMEM((tok_count, d_model), bf16),
            pltpu.VMEM((num_experts, tok_count), jnp.int32),
            pltpu.VMEM((2, capacity, d_model), bf16),
            pltpu.VMEM((dests, capacity, d_model), bf16),
            pltpu.VMEM((dests * capacity, ff), bf16),
            pltpu.VMEM((2, 2, fsdp, d_shard, FFB), bf16),
            pltpu.VMEM((2, ff, d_shard), bf16),
            pltpu.VMEM((dests, capacity, d_shard), bf16),
            dma((len(units), 4)), dma((len(units), 4)),
            dma((local, dests)), dma((local, dests)),
            dma((local, dests)), dma((local, dests)),
            dma((fsdp, dests)), dma((fsdp, dests)),
            dma, dma((2,)), dma((dests,)), dma((2, 2, fsdp)), dma((2,)), dma((2,)),
        ],
        compiler_params=pltpu.CompilerParams(collective_id=0, has_side_effects=True, vmem_limit_bytes=VMEM_LIMIT),
        name='moe_exchange',
    )(top2_ids.T, norm_gain.reshape(1, d_model), w_router.T, hidden, w_gate, w_up, w_down)[:4]


def local_block(hidden, norm_gain, w_router, w_gate, w_up, w_down, top2_ids, *, fsdp, dests):
    tok_local = hidden.shape[0]
    num_experts = w_router.shape[1]
    capacity = (5 * tok_local + 2 * num_experts - 1) // (2 * num_experts)
    ret, tok, plan, slots = exchange(top2_ids, norm_gain, w_router, hidden, w_gate, w_up, w_down, fsdp, dests, capacity)
    return combine(hidden, ret, tok, plan, slots, capacity)


def solution(mesh):
    tok_spec = P(('dp', 'fsdp', 'ep'), None)
    in_specs = (tok_spec, P(None), P(None, None), P('ep', 'fsdp', None), P('ep', 'fsdp', None), P('ep', None, 'fsdp'), tok_spec)
    block = functools.partial(local_block, fsdp=mesh.shape['fsdp'], dests=mesh.shape['ep'])
    return jax.shard_map(block, mesh=mesh, in_specs=in_specs, out_specs=tok_spec, check_vma=False)
```
